32 devices in a mesh: front: 8 (over z, x), panel: 4 (over y, core).
Axes of the slice: x: 2, y: 2, z: 4, core: 2. Of those that a mesh axis runs over, the one named last changes fastest.
Arguments:
- coupling: bfloat16 [8, 2048, 2048], P('front', 'panel'), may hold values from -1 to 1
- pivot_inverse: bfloat16 [8, 2048, 2048], P('front', 'panel'), may hold values from -0.125 to 0.125
- pivots: float32 [8, 2048], P('front'), as said below
- trailing: float32 [8, 2048, 2048], P('front', 'panel'), may hold values from -12 to 12
- sketch: float32 [8, 8, 8, 32, 256], P('front', 'panel'), may hold values from -6 to 6
- extend_map: int32 [8, 2048], replicated, may hold values from 0 to 1023, as said below
- parent_of: int32 [8], replicated, may hold values from 0 to 7, as said below
- parent_base: bfloat16 [8, 4096, 4096], P('front', 'panel'), may hold values from -6 to 6
Outputs:
- assembled: bfloat16 [8, 4096, 4096], P('front', 'panel')
The draws below stay inside these ranges and needn't reach their ends.
Inputs may be any that keep to these rules, and one draw needn't show every extreme that they name: `extend_map`: within each front and each aligned block of 2048 / 4 entries the values are distinct and rising. `pivots`: every entry's magnitude lies between 0.5 and 2 times 2048 ** -0.5; signs are mixed. `parent_of`: no parent has more than 4 children; some parent has exactly 4.
All inputs are finite; a program needn't handle non-finite values.
Results may differ from the reference program's by a relative error of at most 0.0043.
Values may be sent and summed in bfloat16 or wider, within the bound.
No kernel may reach another device: no remote copies, remote signals or barrier semaphores. Data moves between devices by JAX's collectives and lax.ppermute only.
A program may use at most 128 MiB of HBM per device.

```python
import jax
import jax.numpy as jnp
from jax import lax

NP = 2048
NC = 2048
PORDER = 4096
TILE = 256
RANK = 32
MAXKIDS = 4
FRONTS = 8
N_PANEL = 4


def draw_pivots(key, part):
    sign_key, size_key = jax.random.split(jax.random.fold_in(key, 11))
    signs = jnp.where(jax.random.bernoulli(sign_key, 0.5, (FRONTS, NP)), 1.0, -1.0).astype(jnp.float32)
    magnitude = jnp.exp(jax.random.uniform(size_key, (FRONTS, NP), jnp.float32, jnp.log(0.5), jnp.log(2.0)))
    return (signs * magnitude / jnp.sqrt(jnp.float32(NP))).astype(jnp.float32)


def draw_extend_map(key, part):
    row_dev = NC // N_PANEL
    parent_dev = PORDER // N_PANEL
    keys = jax.random.split(jax.random.fold_in(key, 23), FRONTS * N_PANEL)

    def one_block(block_key):
        chosen = jax.random.permutation(block_key, parent_dev)[:row_dev]
        return jnp.sort(chosen).astype(jnp.int32)
    blocks = jax.vmap(one_block)(keys)
    return blocks.reshape(FRONTS, NC).astype(jnp.int32)


def draw_parent_of(key, part):
    base = jax.random.fold_in(key, 41)
    order_key, full_key, rest_key = jax.random.split(base, 3)
    full_parent = jax.random.randint(full_key, (), 0, FRONTS).astype(jnp.int32)
    other_slots = jnp.arange((FRONTS - 1) * MAXKIDS, dtype=jnp.int32) // MAXKIDS
    other_slots = other_slots + (other_slots >= full_parent).astype(jnp.int32)
    shuffled = jax.random.permutation(rest_key, other_slots)
    listing = jnp.concatenate([jnp.full((MAXKIDS,), 1, jnp.int32) * full_parent, shuffled[:FRONTS - MAXKIDS]])
    placing = jax.random.permutation(order_key, FRONTS).astype(jnp.int32)
    return listing[placing].astype(jnp.int32)


def draw_coupling(key, part):
    base = jax.random.fold_in(key, 31)
    tile_rows = NC // TILE
    decay = 1.5 * RANK
    spectrum = jnp.exp(-jnp.arange(TILE, dtype=jnp.float32) / decay)
    scale = jnp.sqrt(jnp.sum(spectrum * spectrum) * NP)

    def one_tile(index):
        left_key, right_key = jax.random.split(jax.random.fold_in(base, index))
        left = jax.random.normal(left_key, (TILE, TILE), jnp.float32)
        right = jax.random.normal(right_key, (TILE, NP), jnp.float32)
        return jnp.dot(left * spectrum[None, :], right, precision=lax.Precision.HIGHEST) / scale
    blocks = lax.map(one_tile, jnp.arange(FRONTS * tile_rows, dtype=jnp.int32))
    return blocks.reshape(FRONTS, NC, NP).astype(jnp.bfloat16)


def draw_trailing(key, part):
    base = jax.random.fold_in(key, 37)
    tile_rows = NC // TILE
    decay = 0.75 * RANK
    spectrum = jnp.exp(-jnp.arange(TILE, dtype=jnp.float32) / decay)
    scale = jnp.sqrt(jnp.sum(spectrum * spectrum))

    def one_tile(index):
        left_key, right_key = jax.random.split(jax.random.fold_in(base, index))
        left = jax.random.normal(left_key, (TILE, TILE), jnp.float32)
        right = jax.random.normal(right_key, (TILE, TILE), jnp.float32)
        return jnp.dot(left * spectrum[None, :], right, precision=lax.Precision.HIGHEST) / scale
    blocks = lax.map(one_tile, jnp.arange(FRONTS * tile_rows * tile_rows, dtype=jnp.int32))
    blocks = blocks.reshape(FRONTS, tile_rows, tile_rows, TILE, TILE)
    return jnp.transpose(blocks, (0, 1, 3, 2, 4)).reshape(FRONTS, NC, NC).astype(jnp.float32)


def level_of(own_key, shape, cuts, smallest, largest):
    def one(axis_at, shards_of):
        steps = jax.random.uniform(jax.random.fold_in(jax.random.fold_in(own_key, 6), axis_at), (shards_of,), jnp.float32, smallest / len(cuts), largest / len(cuts))
        return jnp.repeat(jnp.exp(steps), shape[axis_at] // shards_of).reshape((-1,) + (1,) * (len(shape) - axis_at - 1))

    level = one(*cuts[0])
    for cut in cuts[1:]:
        level = level * one(*cut)
    return level


def bell_draw(stream_key, shape, scale, reach, cuts=(), kind=jnp.bfloat16):
    array = scale * jax.random.normal(stream_key, shape, jnp.float32)
    if cuts:
        array = array * level_of(stream_key, shape, cuts, -0.22, 0.18)
    return jnp.clip(array, -reach, reach).astype(kind)


def setup_inputs(seed: int = 0) -> dict:
    seeds = jax.random.split(jax.random.key(seed), 9)
    return {
        "coupling": draw_coupling(jax.random.fold_in(seeds[8], 71), 0),
        "pivot_inverse": bell_draw(seeds[1], (FRONTS, NP, NP), NP ** -0.5, 0.125, ((0, 8), (1, 4))),
        "pivots": draw_pivots(jax.random.fold_in(seeds[8], 71), 0),
        "trailing": draw_trailing(jax.random.fold_in(seeds[8], 71), 0),
        "sketch": bell_draw(seeds[4], (FRONTS, NC // TILE, NC // TILE, RANK, TILE), 1.0, 6.0, ((0, 8), (1, 4)), jnp.float32),
        "extend_map": draw_extend_map(jax.random.fold_in(seeds[8], 71), 0),
        "parent_of": draw_parent_of(jax.random.fold_in(seeds[8], 71), 0),
        "parent_base": bell_draw(seeds[7], (FRONTS, PORDER, PORDER), 1.0, 6.0, ((0, 8), (1, 4))),
    }


def compress(schur, omega):
    tiles = schur.reshape(NC // TILE, TILE, NC // TILE, TILE)
    range_t = jnp.einsum('ijkb,iajb->ijka', omega, tiles, precision=lax.Precision.HIGHEST)
    gram = jnp.einsum('ijka,ijla->ijkl', range_t, range_t, precision=lax.Precision.HIGHEST)
    lower = jnp.linalg.cholesky(gram)
    basis = jax.scipy.linalg.solve_triangular(lower, range_t, lower=True)
    coeff = jnp.einsum('ijka,iajb->ijkb', basis, tiles, precision=lax.Precision.HIGHEST)
    return (basis.astype(jnp.bfloat16), coeff.astype(jnp.bfloat16))

def expand(basis, coeff):
    dense = jnp.einsum('ijka,ijkb->iajb', basis.astype(jnp.float32), coeff.astype(jnp.float32))
    return dense.reshape(NC, NC)

def reference(coupling, pivot_inverse, pivots, trailing, sketch, extend_map, parent_of, parent_base):
    row_dev = NC // N_PANEL
    parent_dev = PORDER // N_PANEL

    def child(carry, inputs):
        coupling_f, inverse_f, pivots_f, trailing_f, sketch_f = inputs
        factor = jnp.dot(coupling_f.astype(jnp.float32), inverse_f.astype(jnp.float32), preferred_element_type=jnp.float32).astype(jnp.bfloat16)
        scaled = (factor.astype(jnp.float32) / pivots_f[None, :]).astype(jnp.bfloat16)
        update = lax.dot_general(scaled.astype(jnp.float32), factor.astype(jnp.float32), (((1,), (1,)), ((), ())), preferred_element_type=jnp.float32)
        basis, coeff = compress(trailing_f - update, sketch_f)
        return (carry, (basis, coeff))
    _, (basis_all, coeff_all) = lax.scan(child, jnp.int32(0), (coupling, pivot_inverse, pivots, trailing, sketch))
    positions = jnp.arange(NC, dtype=jnp.int32)
    global_map = (positions // row_dev * parent_dev)[None, :] + extend_map.astype(jnp.int32)

    def parent(carry, target):

        def add_child(front_idx, total):

            def place(acc):
                where = global_map[front_idx]
                return acc.at[where[:, None], where[None, :]].add(expand(basis_all[front_idx], coeff_all[front_idx]))
            return lax.cond(parent_of[front_idx] == target, place, lambda acc: acc, total)
        start = parent_base[target].astype(jnp.float32)
        total = lax.fori_loop(0, FRONTS, add_child, start)
        return (carry, total.astype(jnp.bfloat16))
    _, assembled = lax.scan(parent, jnp.int32(0), jnp.arange(FRONTS, dtype=jnp.int32))
    return assembled
```

```python
import functools

import jax
import jax.numpy as jnp
from jax import lax
from jax.experimental import pallas as pl
from jax.experimental.pallas import tpu as pltpu
from jax.sharding import PartitionSpec as P

KIDS = 4
NT = (((1,), (1,)), ((), ()))
NN = (((1,), (0,)), ((), ()))


def halves(x):
    high = x.astype(jnp.bfloat16)
    return high, (x - high.astype(jnp.float32)).astype(jnp.bfloat16)


def dot3(a, b, dims):
    a_hi, a_lo = a
    b_hi, b_lo = b
    mm = functools.partial(lax.dot_general, dimension_numbers=dims, preferred_element_type=jnp.float32)
    return mm(a_hi, b_hi) + (mm(a_hi, b_lo) + mm(a_lo, b_hi))


def compress_kernel(scaled, factor, trailing, omega, basis, coeff, tiles, ranges, grams):
    j = pl.program_id(0)
    tile_rows, tile_cols, rank, size = basis.shape
    update = lax.dot_general(scaled[...], factor[...], NT, preferred_element_type=jnp.float32)
    schur = trailing[...] - update
    for i in range(tile_rows):
        tile = schur[i * size:(i + 1) * size]
        tiles[i, j] = tile
        y = dot3(halves(omega[i, 0]), halves(tile), NT)
        ranges[i, j] = y
        grams[i, j] = lax.dot_general(
            y, y, NT, precision=lax.Precision.HIGHEST, preferred_element_type=jnp.float32
        )

    @pl.when(j == tile_cols - 1)
    def _():
        for i in range(tile_rows):
            row_id = lax.broadcasted_iota(jnp.int32, (tile_cols, rank, rank), 1)
            col_id = lax.broadcasted_iota(jnp.int32, (tile_cols, rank, rank), 2)
            eye = jnp.where(row_id == col_id, 1.0, 0.0).astype(jnp.float32)
            work = jnp.concatenate([grams[i], eye], axis=2)
            rows = lax.broadcasted_iota(jnp.int32, (tile_cols, rank, 1), 1)
            for k in range(rank):
                scale = lax.rsqrt(work[:, k:k + 1, k:k + 1])
                pivot_row = work[:, k:k + 1, :] * scale
                column = work[:, :, k:k + 1] * scale
                below = jnp.where(rows > k, column, 0.0)
                work = jnp.where(rows == k, pivot_row, work - below * pivot_row)
            inverse = work[:, :, rank:]
            for jj in range(tile_cols):
                u = lax.dot_general(
                    inverse[jj], ranges[i, jj], NN,
                    precision=lax.Precision.HIGHEST, preferred_element_type=jnp.float32,
                )
                basis[i, jj] = u.astype(jnp.bfloat16)
                coeff[i, jj] = dot3(halves(u), halves(tiles[i, jj]), NN).astype(jnp.bfloat16)


def compress(scaled, factor, trailing, omega):
    tile_rows, tile_cols, rank, size = omega.shape
    rows, width = scaled.shape
    out = jax.ShapeDtypeStruct(omega.shape, jnp.bfloat16)
    whole = pl.BlockSpec(omega.shape, lambda j: (0, 0, 0, 0))
    return pl.pallas_call(
        compress_kernel,
        grid=(tile_cols,),
        in_specs=[
            pl.BlockSpec((rows, width), lambda j: (0, 0)),
            pl.BlockSpec((size, width), lambda j: (j, 0)),
            pl.BlockSpec((rows, size), lambda j: (0, j)),
            pl.BlockSpec((tile_rows, 1, rank, size), lambda j: (0, j, 0, 0)),
        ],
        out_specs=[whole, whole],
        out_shape=[out, out],
        scratch_shapes=[
            pltpu.VMEM((tile_rows, tile_cols, size, size), jnp.float32),
            pltpu.VMEM(omega.shape, jnp.float32),
            pltpu.VMEM((tile_rows, tile_cols, rank, rank), jnp.float32),
        ],
        compiler_params=pltpu.CompilerParams(vmem_limit_bytes=48 << 20),
        name="compress",
    )(scaled, factor, trailing, omega)


def place_kernel(meta, row_maps, col_maps, basis, coeff, base, out, left, right):
    b = pl.program_id(0)
    tile_rows, tile_cols, rank, size = basis.shape[1:]
    height, width = base.shape
    per_block = col_maps.shape[1] // size
    blocks = tile_cols // per_block
    group = per_block * rank
    depth = tile_rows * group

    def selection(maps, child, t, targets):
        ids = maps[pl.ds(child, 1), t * size:(t + 1) * size]
        hit = lax.broadcasted_iota(jnp.int32, (targets, size), 0) == ids
        return jnp.where(hit, 1.0, 0.0).astype(jnp.bfloat16)

    for slot in range(KIDS):
        child = meta[slot]
        lo = slot * depth

        @pl.when(jnp.logical_and(b == 0, child >= 0))
        def _():
            for i in range(tile_rows):
                pick = selection(row_maps, child, i, height)
                source = basis[child, i].reshape(tile_cols * rank, size)
                spread = lax.dot_general(pick, source, NT, preferred_element_type=jnp.float32)
                spread = spread.astype(jnp.bfloat16)
                for block in range(blocks):
                    at = lo + i * group
                    left[block, :, at:at + group] = spread[:, block * group:(block + 1) * group]

        @pl.when(jnp.logical_and(b == 0, child < 0))
        def _():
            left[:, :, lo:lo + depth] = jnp.zeros((blocks, height, depth), jnp.bfloat16)
            right[:, lo:lo + depth] = jnp.zeros((width, depth), jnp.bfloat16)

        @pl.when(child >= 0)
        def _():
            for t in range(per_block):
                pick = selection(col_maps, child, t, width)
                for i in range(tile_rows):
                    source = coeff[child, i, b * per_block + t]
                    spread = lax.dot_general(pick, source, NT, preferred_element_type=jnp.float32)
                    at = lo + i * group + t * rank
                    right[:, at:at + rank] = spread.astype(jnp.bfloat16)

    total = lax.dot_general(left[b], right[...], NT, preferred_element_type=jnp.float32)
    out[...] = (base[...].astype(jnp.float32) + total).astype(jnp.bfloat16)


def place(meta, extend_map, basis_in, coeff_in, base, row_dev):
    fronts, tile_rows, tile_cols, rank, size = basis_in.shape
    height, full = base.shape
    panels = extend_map.shape[1] // row_dev
    width = full // panels
    whole = pl.BlockSpec(basis_in.shape, lambda b, m: (0, 0, 0, 0, 0))
    depth = KIDS * tile_rows * (row_dev // size) * rank
    return pl.pallas_call(
        place_kernel,
        grid_spec=pltpu.PrefetchScalarGridSpec(
            num_scalar_prefetch=1,
            grid=(panels,),
            in_specs=[
                pl.BlockSpec((fronts, row_dev), lambda b, m: (0, m[KIDS])),
                pl.BlockSpec((fronts, row_dev), lambda b, m: (0, b)),
                whole,
                whole,
                pl.BlockSpec((height, width), lambda b, m: (0, b)),
            ],
            out_specs=pl.BlockSpec((height, width), lambda b, m: (0, b)),
            scratch_shapes=[
                pltpu.VMEM((panels, height, depth), jnp.bfloat16),
                pltpu.VMEM((width, depth), jnp.bfloat16),
            ],
        ),
        out_shape=jax.ShapeDtypeStruct(base.shape, base.dtype),
        compiler_params=pltpu.CompilerParams(vmem_limit_bytes=56 << 20),
        name="place",
    )(meta, extend_map, extend_map, basis_in, coeff_in, base)


def body(coupling, pivot_inverse, pivots, trailing, sketch, extend_map, parent_of, parent_base):
    rows_here = coupling[0]
    row_dev = rows_here.shape[0]
    factor_sum = jnp.dot(
        rows_here,
        lax.all_gather(pivot_inverse, "panel", axis=1, tiled=True)[0],
        preferred_element_type=jnp.float32,
    )
    factor = factor_sum.astype(jnp.bfloat16)
    scaled = (factor.astype(jnp.float32) / pivots[0][None, :]).astype(jnp.bfloat16)
    gathered = lax.all_gather(factor, "panel", axis=0, tiled=True)
    basis, coeff = compress(scaled, gathered, trailing[0], sketch[0])
    owner = lax.axis_index("front")
    panel_here = lax.axis_index("panel").astype(jnp.int32)
    fronts = parent_of.shape[0]
    mine = parent_of == owner
    order = jnp.cumsum(mine.astype(jnp.int32)) - 1
    slots = jnp.arange(KIDS, dtype=jnp.int32)
    match = mine[None, :] & (order[None, :] == slots[:, None])
    child = jnp.sum(jnp.where(match, jnp.arange(fronts, dtype=jnp.int32)[None, :] + 1, 0), axis=1) - 1
    meta = jnp.concatenate([child, panel_here[None]]).astype(jnp.int32)
    basis_in = lax.all_gather(basis[None], "front", axis=0, tiled=True)
    coeff_in = lax.all_gather(coeff[None], "front", axis=0, tiled=True)
    return place(meta, extend_map, basis_in, coeff_in, parent_base[0], row_dev)[None]


def solution(mesh):
    placed = (
        P("front", "panel", None),
        P("front", "panel", None),
        P("front", None),
        P("front", "panel", None),
        P("front", "panel", None, None, None),
        P(),
        P(),
        P("front", "panel", None),
    )
    return jax.shard_map(
        body, mesh=mesh, in_specs=placed, out_specs=P("front", "panel", None), check_vma=False
    )
```

```python
import functools

import jax
import jax.numpy as jnp
from jax import lax
from jax.experimental import pallas as pl
from jax.experimental.pallas import tpu as pltpu
from jax.sharding import PartitionSpec as P

KIDS = 4
NT = (((1,), (1,)), ((), ()))
NN = (((1,), (0,)), ((), ()))


def halves(x):
    high = x.astype(jnp.bfloat16)
    return high, (x - high.astype(jnp.float32)).astype(jnp.bfloat16)


def dot3(a, b, dims):
    a_hi, a_lo = a
    b_hi, b_lo = b
    mm = functools.partial(lax.dot_general, dimension_numbers=dims, preferred_element_type=jnp.float32)
    return mm(a_hi, b_hi) + (mm(a_hi, b_lo) + mm(a_lo, b_hi))


def swap(x, axis, bit):
    return lax.ppermute(x, axis, [(s, s ^ bit) for s in range(lax.axis_size(axis))])


def bits_of(count, lowest):
    bits = []
    bit = count // 2
    while bit >= lowest:
        bits.append(bit)
        bit //= 2
    return bits


def compress_kernel(meta, scaled, *refs, pieces, tile_rows):
    count = len(pieces)
    factors = refs[:count]
    trailings = refs[count:2 * count]
    omegas = refs[2 * count:3 * count]
    out, tiles, ranges, grams = refs[3 * count:]
    rank, size = out.shape[3:]
    total = sum(pieces)
    at = 0
    for n in range(count):
        update = lax.dot_general(scaled[...], factors[n][...], NT, preferred_element_type=jnp.float32)
        schur = trailings[n][...] - update
        for t in range(pieces[n]):
            for i in range(tile_rows):
                tile = schur[i * size:(i + 1) * size, t * size:(t + 1) * size]
                index = at * tile_rows + i
                tiles[index] = tile
                y = dot3(halves(omegas[n][i, t]), halves(tile), NT)
                ranges[index] = y
                grams[index] = lax.dot_general(
                    y, y, NT, precision=lax.Precision.HIGHEST, preferred_element_type=jnp.float32
                )
            at += 1
    batch = total * tile_rows
    row_id = lax.broadcasted_iota(jnp.int32, (batch, rank, rank), 1)
    col_id = lax.broadcasted_iota(jnp.int32, (batch, rank, rank), 2)
    eye = jnp.where(row_id == col_id, 1.0, 0.0).astype(jnp.float32)
    work = jnp.concatenate([grams[...], eye], axis=2)
    rows = lax.broadcasted_iota(jnp.int32, (batch, rank, 1), 1)
    for k in range(rank):
        scale = lax.rsqrt(work[:, k:k + 1, k:k + 1])
        pivot_row = work[:, k:k + 1, :] * scale
        column = work[:, :, k:k + 1] * scale
        below = jnp.where(rows > k, column, 0.0)
        work = jnp.where(rows == k, pivot_row, work - below * pivot_row)
    inverse = work[:, :, rank:]
    at = 0
    for n in range(count):
        for t in range(pieces[n]):
            slot = meta[count + n] + t
            for i in range(tile_rows):
                index = at * tile_rows + i
                u = lax.dot_general(
                    inverse[index], ranges[index], NN,
                    precision=lax.Precision.HIGHEST, preferred_element_type=jnp.float32,
                )
                out[0, i, slot] = u.astype(jnp.bfloat16)
                out[1, i, slot] = dot3(halves(u), halves(tiles[index]), NN).astype(jnp.bfloat16)
            at += 1


def compress(scaled, trailing, omega, parts):
    tile_rows, tile_cols, rank, size = omega.shape
    rows, width = scaled.shape
    pieces = tuple(part[0].shape[0] // size for part in parts)
    total = sum(pieces)
    count = len(parts)
    meta = jnp.stack([part[1] for part in parts] + [jnp.int32(0) + part[2] for part in parts]).astype(jnp.int32)
    in_specs = [pl.BlockSpec((rows, width), lambda g, m: (0, 0))]
    in_specs += [pl.BlockSpec(part[0].shape, lambda g, m: (0, 0)) for part in parts]
    for n in range(count):
        in_specs.append(pl.BlockSpec((rows, pieces[n] * size), lambda g, m, n=n: (0, m[n])))
    for n in range(count):
        in_specs.append(pl.BlockSpec((tile_rows, pieces[n], rank, size), lambda g, m, n=n: (0, m[n], 0, 0)))
    out = jax.ShapeDtypeStruct((2, tile_rows, total, rank, size), jnp.bfloat16)
    batch = total * tile_rows
    flops = 2 * rows * width * total * size
    return pl.pallas_call(
        functools.partial(compress_kernel, pieces=pieces, tile_rows=tile_rows),
        grid_spec=pltpu.PrefetchScalarGridSpec(
            num_scalar_prefetch=1,
            grid=(1,),
            in_specs=in_specs,
            out_specs=pl.BlockSpec(out.shape, lambda g, m: (0, 0, 0, 0, 0)),
            scratch_shapes=[
                pltpu.VMEM((batch, size, size), jnp.float32),
                pltpu.VMEM((batch, rank, size), jnp.float32),
                pltpu.VMEM((batch, rank, rank), jnp.float32),
            ],
        ),
        out_shape=out,
        compiler_params=pltpu.CompilerParams(vmem_limit_bytes=40 << 20),
        cost_estimate=pl.CostEstimate(flops=4 * flops, transcendentals=0, bytes_accessed=8 * rows * width),
        name="compress",
    )(meta, scaled, *[part[0] for part in parts], *[trailing] * count, *[omega] * count)


def place_kernel(meta, row_maps, col_maps, packs, base, *rest):
    out, left, right = rest[-3:]
    g = pl.program_id(0)
    fronts, kinds, tile_rows, total, rank, size = packs.shape
    height, width = base.shape
    per_block = col_maps.shape[1] // size
    group = per_block * rank
    depth = tile_rows * group

    def selection(maps, child, t, targets):
        ids = maps[pl.ds(child, 1), t * size:(t + 1) * size]
        hit = lax.broadcasted_iota(jnp.int32, (targets, size), 0) == ids
        return jnp.where(hit, 1.0, 0.0).astype(jnp.bfloat16)

    for slot in range(KIDS):
        child = meta[slot]
        offset = meta[KIDS + slot]
        lo = slot * depth

        @pl.when(child < 0)
        def _():
            left[:, lo:lo + depth] = jnp.zeros((height, depth), jnp.bfloat16)
            right[:, lo:lo + depth] = jnp.zeros((width, depth), jnp.bfloat16)

        @pl.when(child >= 0)
        def _():
            for i in range(tile_rows):
                pick = selection(row_maps, child, i, height)
                source = packs[offset, 0, i, pl.ds(g * per_block, per_block)].reshape(group, size)
                spread = lax.dot_general(pick, source, NT, preferred_element_type=jnp.float32)
                at = lo + i * group
                left[:, at:at + group] = spread.astype(jnp.bfloat16)
            for t in range(per_block):
                pick = selection(col_maps, child, t, width)
                for i in range(tile_rows):
                    source = packs[offset, 1, i, g * per_block + t]
                    spread = lax.dot_general(pick, source, NT, preferred_element_type=jnp.float32)
                    at = lo + i * group + t * rank
                    right[:, at:at + rank] = spread.astype(jnp.bfloat16)

    total_sum = lax.dot_general(left[...], right[...], NT, preferred_element_type=jnp.float32)
    out[...] = (base[...].astype(jnp.float32) + total_sum).astype(jnp.bfloat16)


def place(meta, extend_map, packs, base, row_dev, blocks, previous):
    fronts, kinds, tile_rows, total, rank, size = packs.shape
    height, full = base.shape
    panels = extend_map.shape[1] // row_dev
    width = full // panels
    depth = KIDS * tile_rows * (row_dev // size) * rank
    first = 2 * KIDS + 1
    in_specs = [
        pl.BlockSpec((fronts, row_dev), lambda g, m: (0, m[2 * KIDS])),
        pl.BlockSpec((fronts, row_dev), lambda g, m: (0, m[first + g])),
        pl.BlockSpec(packs.shape, lambda g, m: (0, 0, 0, 0, 0, 0)),
        pl.BlockSpec((height, width), lambda g, m: (0, m[first + g])),
    ]
    operands = [extend_map, extend_map, packs, base]
    aliases = {}
    if previous is not None:
        in_specs.append(pl.BlockSpec(memory_space=pl.ANY))
        operands.append(previous)
        aliases = {len(operands): 0}
    flops = 2 * height * width * depth * blocks
    return pl.pallas_call(
        place_kernel,
        grid_spec=pltpu.PrefetchScalarGridSpec(
            num_scalar_prefetch=1,
            grid=(blocks,),
            in_specs=in_specs,
            out_specs=pl.BlockSpec((height, width), lambda g, m: (0, m[first + g])),
            scratch_shapes=[
                pltpu.VMEM((height, depth), jnp.bfloat16),
                pltpu.VMEM((width, depth), jnp.bfloat16),
            ],
        ),
        out_shape=jax.ShapeDtypeStruct(base.shape, base.dtype),
        input_output_aliases=aliases,
        compiler_params=pltpu.CompilerParams(vmem_limit_bytes=48 << 20),
        cost_estimate=pl.CostEstimate(flops=4 * flops, transcendentals=0, bytes_accessed=4 * height * width * blocks),
        name="place",
    )(meta, *operands)


def gather_fronts(pack):
    held = {0: pack}
    for bit in bits_of(lax.axis_size("front"), 1):
        for offset in list(held):
            held[offset ^ bit] = swap(held[offset], "front", bit)
    return jnp.stack([held[offset] for offset in range(len(held))])


def body(coupling, pivot_inverse, pivots, trailing, sketch, extend_map, parent_of, parent_base):
    rows_here = coupling[0]
    inverse = pivot_inverse[0]
    row_dev = rows_here.shape[0]
    omega = sketch[0]
    tile_rows, tile_cols, rank, size = omega.shape
    panels = lax.axis_size("panel")
    panel_here = lax.axis_index("panel").astype(jnp.int32)
    owner = lax.axis_index("front").astype(jnp.int32)
    core = panel_here & 1
    far_bits = bits_of(panels, 2)

    splits = 2
    step = row_dev // splits
    held = {0: [inverse[n * step:(n + 1) * step] for n in range(splits)]}
    for bit in far_bits:
        for offset in list(held):
            held[offset ^ bit] = [swap(x, "panel", bit) for x in held[offset]]
    total = None
    for offset in list(held):
        if offset == 0:
            held[1] = [swap(inverse, "panel", 1)]
        else:
            held[offset ^ 1] = [swap(x, "panel", 1) for x in held[offset]]
    held[0] = [inverse]
    for offset in sorted(held):
        source = (panel_here ^ offset) * row_dev
        for n, x in enumerate(held[offset]):
            part = lax.dynamic_slice_in_dim(rows_here, source + n * x.shape[0], x.shape[0], 1)
            term = jnp.dot(part, x, preferred_element_type=jnp.float32)
            total = term if total is None else total + term
    factor = total.astype(jnp.bfloat16)
    scaled = (factor.astype(jnp.float32) / pivots[0][None, :]).astype(jnp.bfloat16)

    fronts = parent_of.shape[0]
    mine = parent_of == owner
    order = jnp.cumsum(mine.astype(jnp.int32)) - 1
    slots = jnp.arange(KIDS, dtype=jnp.int32)
    match = mine[None, :] & (order[None, :] == slots[:, None])
    child = jnp.sum(jnp.where(match, jnp.arange(fronts, dtype=jnp.int32)[None, :] + 1, 0), axis=1) - 1
    slot_meta = jnp.concatenate([child, jnp.maximum(child, 0) ^ owner, panel_here[None]]).astype(jnp.int32)

    near = swap(factor, "panel", 1)
    per_block = row_dev // size
    chunks = [([panel_here, panel_here ^ 1], [(factor, panel_here, 0), (near, panel_here ^ 1, per_block)])]
    if per_block % 2 == 0:
        half = row_dev // 2
        own_pair = jnp.where(core == 0, 0, 1)
        pieces = []
        for c in range(2):
            chosen = jnp.where(
                own_pair == c,
                lax.dynamic_slice_in_dim(factor, core * half, half, 0),
                lax.dynamic_slice_in_dim(near, core * half, half, 0),
            )
            held = {0: chosen}
            for bit in far_bits:
                for offset in list(held):
                    held[offset ^ bit] = swap(held[offset], "panel", bit)
            pieces.append(held)
        for offset in sorted(pieces[0])[1:]:
            for c in range(2):
                here = pieces[c][offset]
                there = swap(here, "panel", 1)
                block = ((panel_here ^ offset) & ~1) + c
                slot_here = core * (per_block // 2)
                slot_there = (1 - core) * (per_block // 2)
                chunks.append((
                    [block],
                    [(here, 2 * block + core, slot_here), (there, 2 * block + 1 - core, slot_there)],
                ))
    else:
        held = {0: factor}
        for bit in far_bits:
            for offset in list(held):
                held[offset ^ bit] = swap(held[offset], "panel", bit)
        for offset in sorted(held)[1:]:
            block = panel_here ^ offset
            there = swap(held[offset], "panel", 1)
            chunks.append(([block, block ^ 1], [(held[offset], block, 0), (there, block ^ 1, per_block)]))

    assembled = None
    for blocks, parts in chunks:
        pack = compress(scaled, trailing[0], omega, parts)
        packs = gather_fronts(pack)
        meta = jnp.concatenate([slot_meta, jnp.stack(blocks).astype(jnp.int32)])
        assembled = place(meta, extend_map, packs, parent_base[0], row_dev, len(blocks), assembled)
    return assembled[None]


def solution(mesh):
    placed = (
        P("front", "panel", None),
        P("front", "panel", None),
        P("front", None),
        P("front", "panel", None),
        P("front", "panel", None, None, None),
        P(),
        P(),
        P("front", "panel", None),
    )
    return jax.shard_map(
        body, mesh=mesh, in_specs=placed, out_specs=P("front", "panel", None), check_vma=False
    )
```

```python
import functools

import jax
import jax.numpy as jnp
from jax import lax
from jax.experimental import pallas as pl
from jax.experimental.pallas import tpu as pltpu
from jax.sharding import PartitionSpec as P


KIDS = 4
NT = (((1,), (1,)), ((), ()))
NN = (((1,), (0,)), ((), ()))


VMEM = pl.BlockSpec(memory_space=pltpu.VMEM)
SMEM = pl.BlockSpec(memory_space=pltpu.SMEM)
HBM = pl.BlockSpec(memory_space=pltpu.HBM)


def in_hbm(arrays):
    return [pltpu.with_memory_space_constraint(x, pltpu.HBM) for x in arrays]


def mm(a, b, dims):
    return lax.dot_general(a, b, dims, preferred_element_type=jnp.float32)


def halves(x):
    high = x.astype(jnp.bfloat16)
    return high, (x - high.astype(jnp.float32)).astype(jnp.bfloat16)


def dot3(a, b, dims):
    a_hi, a_lo = a
    b_hi, b_lo = b
    rows = a_hi.shape[0]
    both = mm(jnp.concatenate([a_hi, a_lo], axis=0), b_hi, dims)
    return both[:rows] + (mm(a_hi, b_lo, dims) + both[rows:])


def swap(x, axis, bit):
    return lax.ppermute(x, axis, [(s, s ^ bit) for s in range(lax.axis_size(axis))])


def bits_of(count, lowest):
    bits = []
    bit = count // 2
    while bit >= lowest:
        bits.append(bit)
        bit //= 2
    return bits


def factor_kernel(meta, coupling, pivots, *refs, first):
    *inverses, factor, scaled = refs
    width = factor.shape[1]
    total = None
    for n, inverse in enumerate(inverses):
        rows = inverse.shape[0]
        at = pl.multiple_of(meta[n] * rows, rows)
        lo = first if inverse.shape[1] > width else 0
        term = mm(coupling[:, pl.ds(at, rows)], inverse[:, lo:lo + width], NN)
        total = term if total is None else total + term
    rounded = total.astype(jnp.bfloat16)
    factor[...] = rounded
    scaled[...] = (rounded.astype(jnp.float32) / pivots[:, first:first + width]).astype(jnp.bfloat16)


def factor_columns(meta, coupling, pivots, inverses, first, width):
    rows = coupling.shape[0]
    out = jax.ShapeDtypeStruct((rows, width), jnp.bfloat16)
    return pl.pallas_call(
        functools.partial(factor_kernel, first=first),
        in_specs=[SMEM] + [VMEM] * (2 + len(inverses)),
        out_specs=[VMEM, VMEM],
        out_shape=[out, out],
        compiler_params=pltpu.CompilerParams(vmem_limit_bytes=32 << 20),
        cost_estimate=pl.CostEstimate(
            flops=2 * rows * coupling.shape[1] * out.shape[1], transcendentals=0, bytes_accessed=1 << 22
        ),
        name="factor",
    )(meta, coupling, pivots, *inverses)


def compress_kernel(meta, *refs, pieces, choices):
    count = len(pieces)
    scaled_a, scaled_b, trailing, omega = refs[:4]
    firsts = []
    at = 4
    for n in range(count):
        firsts.append(refs[at:at + choices[n]])
        at += choices[n]
    seconds = refs[at:at + count]
    out, left_a, left_b = refs[at + count:at + count + 3]
    local = refs[at + count + 3:at + count + 3 + 4 * count]
    tiles, ranges, grams, sems = refs[at + count + 3 + 4 * count:]
    tile_rows, rank, size = omega.shape[0], omega.shape[2], omega.shape[3]
    batch = sum(pieces) * tile_rows

    def copies(n, which):
        first, second, old, draws = local[4 * n:4 * n + 4]
        start = pl.multiple_of(meta[4 * n] * size, size)
        column = meta[4 * n + 1]
        left = pl.multiple_of(column * size, size)
        span = pieces[n] * size
        sem = 2 + 4 * n
        source, target = (
            (lambda x: firsts[n][x].at[pl.ds(start, span)], first),
            (lambda x: seconds[n], second),
            (lambda x: trailing.at[:, pl.ds(left, span)], old),
            (lambda x: omega.at[:, pl.ds(column, pieces[n])], draws),
        )[which]
        return lambda x=0: pltpu.make_async_copy(source(x), target, sems.at[sem + which])

    def start_copies(n, which):
        make = copies(n, which)
        if which > 0 or choices[n] == 1:
            make().start()
        else:
            for x in range(choices[n]):
                @pl.when(meta[4 * n + 3] == x)
                def _():
                    make(x).start()

    scaled_copies = (
        pltpu.make_async_copy(scaled_a, left_a, sems.at[0]),
        pltpu.make_async_copy(scaled_b, left_b, sems.at[1]),
    )
    scaled_copies[0].start()
    start_copies(0, 0)
    scaled_copies[1].start()
    for n in range(count):
        for which in range(4):
            if n > 0 or which > 0:
                start_copies(n, which)

    at = 0
    for n in range(count):
        first, second, old, draws = local[4 * n:4 * n + 4]
        if n == 0:
            scaled_copies[0].wait()
        copies(n, 0)().wait()
        update = mm(left_a[...], first[...], NT)
        if n == 0:
            scaled_copies[1].wait()
        copies(n, 1)().wait()
        update = update + mm(left_b[...], second[...], NT)
        copies(n, 2)().wait()
        schur = old[...] - update
        copies(n, 3)().wait()
        for t in range(pieces[n]):
            for i in range(tile_rows):
                tile = schur[i * size:(i + 1) * size, t * size:(t + 1) * size]
                tiles[at] = tile
                y = dot3(halves(draws[i, t]), halves(tile), NT)
                ranges[at] = y
                grams[at] = lax.dot_general(
                    y, y, NT, precision=lax.Precision.HIGHEST, preferred_element_type=jnp.float32
                )
                at += 1
    row_id = lax.broadcasted_iota(jnp.int32, (batch, rank, rank), 1)
    col_id = lax.broadcasted_iota(jnp.int32, (batch, rank, rank), 2)
    eye = jnp.where(row_id == col_id, 1.0, 0.0).astype(jnp.float32)
    work = jnp.concatenate([grams[...], eye], axis=2)
    rows = lax.broadcasted_iota(jnp.int32, (batch, rank, 1), 1)
    for k in range(rank):
        scale = lax.rsqrt(work[:, k:k + 1, k:k + 1])
        pivot_row = work[:, k:k + 1, :] * scale
        column = work[:, :, k:k + 1] * scale
        below = jnp.where(rows > k, column, 0.0)
        work = jnp.where(rows == k, pivot_row, work - below * pivot_row)
    inverse = work[:, :, rank:]
    at = 0
    for n in range(count):
        for t in range(pieces[n]):
            slot = meta[4 * n + 2] + t
            for i in range(tile_rows):
                u = lax.dot_general(
                    inverse[at], ranges[at], NN,
                    precision=lax.Precision.HIGHEST, preferred_element_type=jnp.float32,
                )
                out[0, i, slot] = u.astype(jnp.bfloat16)
                out[1, i, slot] = dot3(halves(u), halves(tiles[at]), NN).astype(jnp.bfloat16)
                at += 1


def compress(scaled, trailing, omega, parts):
    tile_rows, _, rank, size = omega.shape
    rows, width = trailing.shape
    pieces = tuple(part[3].shape[0] // size for part in parts)
    choices = tuple(len(part[0]) for part in parts)
    total = sum(pieces)
    meta = jnp.stack(
        [jnp.int32(0) + x for part in parts for x in (part[2], part[4], part[5], part[1])]
    ).astype(jnp.int32)
    out = jax.ShapeDtypeStruct((2, tile_rows, total, rank, size), jnp.bfloat16)
    batch = total * tile_rows
    operands = [*scaled, trailing, omega]
    local = []
    for part, piece in zip(parts, pieces):
        operands += part[0]
        local += [
            pltpu.VMEM((piece * size, part[0][0].shape[1]), jnp.bfloat16),
            pltpu.VMEM(part[3].shape, jnp.bfloat16),
            pltpu.VMEM((rows, piece * size), jnp.float32),
            pltpu.VMEM((tile_rows, piece, rank, size), jnp.float32),
        ]
    operands += [part[3] for part in parts]
    return pl.pallas_call(
        functools.partial(compress_kernel, pieces=pieces, choices=choices),
        in_specs=[SMEM] + [HBM] * len(operands),
        out_specs=VMEM,
        out_shape=out,
        scratch_shapes=[pltpu.VMEM(x.shape, jnp.bfloat16) for x in scaled] + local + [
            pltpu.VMEM((batch, size, size), jnp.float32),
            pltpu.VMEM((batch, rank, size), jnp.float32),
            pltpu.VMEM((batch, rank, rank), jnp.float32),
            pltpu.SemaphoreType.DMA((2 + 4 * len(parts),)),
        ],
        compiler_params=pltpu.CompilerParams(vmem_limit_bytes=40 << 20),
        cost_estimate=pl.CostEstimate(
            flops=8 * rows * width * total * size, transcendentals=0, bytes_accessed=8 * rows * width
        ),
        name="compress",
    )(meta, *in_hbm(operands))


def place_kernel(meta, maps, base, *refs, fronts, blocks, row_dev):
    count = len(blocks)
    packs = [refs[n * fronts:(n + 1) * fronts] for n in range(count)]
    out, *mine = refs[-(5 + count):-4]
    lines, left, right, sems = refs[-4:]
    _, tile_rows, _, rank, size = packs[0][0].shape
    steps, height, width = lines.shape
    per_block = row_dev // size
    group = per_block * rank
    depth = tile_rows * group
    spare = height - row_dev

    def fetch(n, slot, go):
        for offset in range(fronts):
            @pl.when(jnp.logical_and(meta[slot] >= 0, meta[KIDS + slot] == offset))
            def _():
                go(pltpu.make_async_copy(packs[n][offset], mine[n].at[slot], sems.at[n * KIDS + slot]))

    def columns(step):
        return pl.ds(pl.multiple_of(meta[2 * KIDS + 1 + step] * width, width), width)

    def load(step):
        return pltpu.make_async_copy(base.at[:, columns(step)], lines.at[step], sems.at[count * KIDS + step])

    def store(step):
        return pltpu.make_async_copy(lines.at[step], out.at[:, columns(step)], sems.at[count * KIDS + steps + step])

    def selection(panel, child, t):
        lane = pl.multiple_of(panel * row_dev + t * size, size)
        ids = maps[pl.ds(child, 1), pl.ds(lane, size)] - t * size
        hit = lax.broadcasted_iota(jnp.int32, (size + spare, size), 0) == ids
        return jnp.where(hit, 1.0, 0.0).astype(jnp.bfloat16)

    for n in range(count):
        for slot in range(KIDS):
            fetch(n, slot, lambda copy: copy.start())
    for step in range(steps):
        load(step).start()
    left[...] = jnp.zeros(left.shape, left.dtype)
    right[...] = jnp.zeros(right.shape, right.dtype)
    for n in range(count):
        for slot in range(KIDS):
            fetch(n, slot, lambda copy: copy.wait())
    for slot in range(KIDS):
        lo = slot * depth

        @pl.when(meta[slot] >= 0)
        def _():
            for i in range(tile_rows):
                source = jnp.concatenate(
                    [mine[n][slot, 0, i].reshape(blocks[n] * group, size) for n in range(count)], axis=0
                )
                spread = mm(selection(meta[2 * KIDS], meta[slot], i), source, NT).astype(jnp.bfloat16)
                for step in range(steps):
                    left[step, i * size:(i + 1) * size + spare, lo + i * group:lo + (i + 1) * group] = (
                        spread[:, step * group:(step + 1) * group]
                    )

    step = 0
    for n in range(count):
        for b in range(blocks[n]):
            for slot in range(KIDS):
                lo = slot * depth

                @pl.when(meta[slot] >= 0)
                def _():
                    for t in range(per_block):
                        source = jnp.concatenate(
                            [mine[n][slot, 1, i, b * per_block + t] for i in range(tile_rows)], axis=0
                        )
                        pick = selection(meta[2 * KIDS + 1 + step], meta[slot], t)
                        spread = mm(pick, source, NT).astype(jnp.bfloat16)
                        for i in range(tile_rows):
                            at = lo + i * group + t * rank
                            right[t * size:(t + 1) * size + spare, at:at + rank] = (
                                spread[:, i * rank:(i + 1) * rank]
                            )

            load(step).wait()
            lines[step] = (
                lines[step].astype(jnp.float32) + mm(left[step], right[...], NT)
            ).astype(jnp.bfloat16)
            store(step).start()
            step += 1
    for step in range(steps):
        store(step).wait()


def place(meta, extend_map, packs, base, row_dev, blocks, previous):
    fronts = len(packs[0])
    _, tile_rows, _, rank, size = packs[0][0].shape
    height, full = base.shape
    panels = extend_map.shape[1] // row_dev
    width = full // panels
    depth = KIDS * tile_rows * (row_dev // size) * rank
    steps = sum(blocks)
    operands = [base] + [x for chunk in packs for x in chunk]
    aliases = {}
    if previous is not None:
        operands.append(previous)
        aliases = {1 + len(operands): 0}
    return pl.pallas_call(
        functools.partial(place_kernel, fronts=fronts, blocks=blocks, row_dev=row_dev),
        in_specs=[SMEM, VMEM] + [HBM] * len(operands),
        out_specs=HBM,
        out_shape=jax.ShapeDtypeStruct(base.shape, base.dtype),
        scratch_shapes=[pltpu.VMEM((KIDS,) + chunk[0].shape, jnp.bfloat16) for chunk in packs] + [
            pltpu.VMEM((steps, height, width), jnp.bfloat16),
            pltpu.VMEM((steps, height, depth), jnp.bfloat16),
            pltpu.VMEM((width, depth), jnp.bfloat16),
            pltpu.SemaphoreType.DMA((len(packs) * KIDS + 2 * steps,)),
        ],
        input_output_aliases=aliases,
        compiler_params=pltpu.CompilerParams(vmem_limit_bytes=48 << 20),
        cost_estimate=pl.CostEstimate(
            flops=8 * height * width * steps * depth, transcendentals=0, bytes_accessed=4 * height * width * steps
        ),
        name="place",
    )(meta, extend_map, *in_hbm(operands))


def spread_panels(x, lowest):
    held = {0: x}
    for bit in bits_of(lax.axis_size("panel"), lowest):
        for offset in list(held):
            held[offset ^ bit] = swap(held[offset], "panel", bit)
    return held


def gather_fronts(pack):
    held = {0: pack}
    for bit in bits_of(lax.axis_size("front"), 1):
        for offset in list(held):
            held[offset ^ bit] = swap(held[offset], "front", bit)
    return [held[offset] for offset in range(len(held))]


def body(coupling, pivot_inverse, pivots, trailing, sketch, extend_map, parent_of, parent_base):
    rows_here = coupling[0]
    inverse = pivot_inverse[0]
    row_dev, width = rows_here.shape
    omega = sketch[0]
    size = omega.shape[3]
    panels = lax.axis_size("panel")
    panel_here = lax.axis_index("panel").astype(jnp.int32)
    owner = lax.axis_index("front").astype(jnp.int32)
    core = panel_here & 1
    per_block = row_dev // size
    middle = inverse.shape[1] // 2

    near_inverse = swap(inverse, "panel", 1)
    held_a = spread_panels(inverse[:, :middle], 2)
    held_b = spread_panels(lax.optimization_barrier(inverse)[:, middle:], 2)
    offsets = range(panels)
    panel_of = jnp.stack([panel_here ^ offset for offset in offsets])

    def columns(held, lo, hi):
        parts = []
        for offset in offsets:
            if offset == 0:
                parts.append(inverse)
            elif offset == 1:
                parts.append(near_inverse)
            elif offset & 1:
                parts.append(swap(held[offset ^ 1], "panel", 1))
            else:
                parts.append(held[offset])
        return factor_columns(panel_of, rows_here, pivots, parts, lo, hi - lo)

    factor_a, scaled_a = columns(held_a, 0, middle)
    far_a = spread_panels(factor_a, 2)
    near_a = {offset ^ 1: swap(x, "panel", 1) for offset, x in far_a.items()}
    first = {**far_a, **near_a}
    factor_b, scaled_b = columns(held_b, middle, width)
    near_b = swap(factor_b, "panel", 1)
    scaled = (scaled_a, scaled_b)

    fronts = parent_of.shape[0]
    mine = parent_of == owner
    rank_of = jnp.cumsum(mine.astype(jnp.int32)) - 1
    slots = jnp.arange(KIDS, dtype=jnp.int32)
    match = mine[None, :] & (rank_of[None, :] == slots[:, None])
    child = jnp.sum(jnp.where(match, jnp.arange(fronts, dtype=jnp.int32)[None, :] + 1, 0), axis=1) - 1
    slot_meta = jnp.concatenate([child, jnp.maximum(child, 0) ^ owner, panel_here[None]]).astype(jnp.int32)

    mate = panel_here ^ 1
    chunks = [(
        [panel_here, mate],
        [
            ([factor_a], 0, 0, factor_b, panel_here * per_block, 0),
            ([first[1]], 0, 0, near_b, mate * per_block, per_block),
        ],
    )]
    if per_block % 2 == 0:
        half = row_dev // 2
        tiles = per_block // 2
        pieces = []
        for c in range(2):
            chosen = jnp.where(
                core == c,
                lax.dynamic_slice_in_dim(factor_b, core * half, half, 0),
                lax.dynamic_slice_in_dim(near_b, core * half, half, 0),
            )
            pieces.append(spread_panels(chosen, 2))
        for offset in sorted(pieces[0])[1:]:
            for c in range(2):
                here = pieces[c][offset]
                there = swap(here, "panel", 1)
                block = ((panel_here ^ offset) & ~1) + c
                both = [first[offset], first[offset ^ 1]]
                parts = [
                    (both, core ^ c, x * tiles, piece, block * per_block + x * tiles, x * tiles)
                    for x, piece in ((core, here), (1 - core, there))
                ]
                chunks.append(([block], parts))
    else:
        held = spread_panels(factor_b, 2)
        for offset in sorted(held)[1:]:
            block = panel_here ^ offset
            there = swap(held[offset], "panel", 1)
            chunks.append((
                [block, block ^ 1],
                [
                    ([first[offset]], 0, 0, held[offset], block * per_block, 0),
                    ([first[offset ^ 1]], 0, 0, there, (block ^ 1) * per_block, per_block),
                ],
            ))

    packs = []
    for _, parts in chunks:
        packs.append(compress(scaled, trailing[0], omega, parts))
    gathered = []
    for pack in packs:
        gathered.append(gather_fronts(pack))
    assembled = None
    for picked in (slice(0, 1), slice(1, None)):
        steps = [block for blocks, _ in chunks[picked] for block in blocks]
        meta = jnp.concatenate([slot_meta, jnp.stack(steps).astype(jnp.int32)])
        counts = tuple(len(blocks) for blocks, _ in chunks[picked])
        assembled = place(meta, extend_map, gathered[picked], parent_base[0], row_dev, counts, assembled)
    return assembled[None]


def solution(mesh):
    placed = (
        P("front", "panel", None),
        P("front", "panel", None),
        P("front", None),
        P("front", "panel", None),
        P("front", "panel", None, None, None),
        P(),
        P(),
        P("front", "panel", None),
    )
    return jax.shard_map(body, mesh=mesh, in_specs=placed, out_specs=P("front", "panel", None), check_vma=False)
```

```python
import functools

import jax
import jax.numpy as jnp
from jax import lax
from jax.experimental import pallas as pl
from jax.experimental.pallas import tpu as pltpu
from jax.sharding import PartitionSpec as P


KIDS = 4
NT = (((1,), (1,)), ((), ()))
NN = (((1,), (0,)), ((), ()))


VMEM = pl.BlockSpec(memory_space=pltpu.VMEM)
SMEM = pl.BlockSpec(memory_space=pltpu.SMEM)
HBM = pl.BlockSpec(memory_space=pltpu.HBM)


def in_hbm(arrays):
    return [pltpu.with_memory_space_constraint(x, pltpu.HBM) for x in arrays]


def mm(a, b, dims):
    return lax.dot_general(a, b, dims, preferred_element_type=jnp.float32)


def halves(x):
    high = x.astype(jnp.bfloat16)
    return high, (x - high.astype(jnp.float32)).astype(jnp.bfloat16)


def dot3(a, b, dims):
    a_hi, a_lo = a
    b_hi, b_lo = b
    rows = a_hi.shape[0]
    both = mm(jnp.concatenate([a_hi, a_lo], axis=0), b_hi, dims)
    return both[:rows] + (mm(a_hi, b_lo, dims) + both[rows:])


def swap(x, axis, bit):
    return lax.ppermute(x, axis, [(s, s ^ bit) for s in range(lax.axis_size(axis))])


def bits_of(count, lowest):
    bits = []
    bit = count // 2
    while bit >= lowest:
        bits.append(bit)
        bit //= 2
    return bits


def factor_kernel(meta, coupling, *refs, first, width, count, early, final):
    total = refs[count][...] if early else None
    for n, inverse in enumerate(refs[:count]):
        rows = inverse.shape[0]
        at = pl.multiple_of(meta[n] * rows, rows)
        lo = first if inverse.shape[1] > width else 0
        term = mm(coupling[:, pl.ds(at, rows)], inverse[:, lo:lo + width], NN)
        total = term if total is None else total + term
    if not final:
        refs[-1][...] = total
        return
    pivots, factor, scaled = refs[-3:]
    rounded = total.astype(jnp.bfloat16)
    factor[...] = rounded
    scaled[...] = (rounded.astype(jnp.float32) / pivots[:, first:first + width]).astype(jnp.bfloat16)


def factor_columns(meta, coupling, inverses, first, width, early=None, pivots=None):
    rows = coupling.shape[0]
    final = pivots is not None
    out = jax.ShapeDtypeStruct((rows, width), jnp.bfloat16 if final else jnp.float32)
    operands = list(inverses) + ([early] if early is not None else []) + ([pivots] if final else [])
    return pl.pallas_call(
        functools.partial(
            factor_kernel, first=first, width=width, count=len(inverses), early=early is not None, final=final
        ),
        in_specs=[SMEM] + [VMEM] * (1 + len(operands)),
        out_specs=[VMEM, VMEM] if final else VMEM,
        out_shape=[out, out] if final else out,
        compiler_params=pltpu.CompilerParams(vmem_limit_bytes=32 << 20),
        cost_estimate=pl.CostEstimate(
            flops=2 * rows * sum(x.shape[0] for x in inverses) * width, transcendentals=0, bytes_accessed=1 << 22
        ),
        name="factor",
    )(meta, coupling, *operands)


def compress_kernel(meta, *refs, pieces, choices):
    count = len(pieces)
    scaled_a, scaled_b, trailing, omega = refs[:4]
    firsts = []
    at = 4
    for n in range(count):
        firsts.append(refs[at:at + choices[n]])
        at += choices[n]
    seconds = refs[at:at + count]
    out, left_a, left_b = refs[at + count:at + count + 3]
    local = refs[at + count + 3:at + count + 3 + 4 * count]
    tiles, ranges, grams, sems = refs[at + count + 3 + 4 * count:]
    tile_rows, rank, size = omega.shape[0], omega.shape[2], omega.shape[3]
    batch = sum(pieces) * tile_rows

    def copies(n, which):
        first, second, old, draws = local[4 * n:4 * n + 4]
        start = pl.multiple_of(meta[4 * n] * size, size)
        column = meta[4 * n + 1]
        left = pl.multiple_of(column * size, size)
        span = pieces[n] * size
        sem = 2 + 4 * n
        source, target = (
            (lambda x: firsts[n][x].at[pl.ds(start, span)], first),
            (lambda x: seconds[n], second),
            (lambda x: trailing.at[:, pl.ds(left, span)], old),
            (lambda x: omega.at[:, pl.ds(column, pieces[n])], draws),
        )[which]
        return lambda x=0: pltpu.make_async_copy(source(x), target, sems.at[sem + which])

    def start_copies(n, which):
        make = copies(n, which)
        if which > 0 or choices[n] == 1:
            make().start()
        else:
            for x in range(choices[n]):
                @pl.when(meta[4 * n + 3] == x)
                def _():
                    make(x).start()

    scaled_copies = (
        pltpu.make_async_copy(scaled_a, left_a, sems.at[0]),
        pltpu.make_async_copy(scaled_b, left_b, sems.at[1]),
    )
    scaled_copies[0].start()
    start_copies(0, 0)
    scaled_copies[1].start()
    for n in range(count):
        for which in range(4):
            if n > 0 or which > 0:
                start_copies(n, which)

    at = 0
    for n in range(count):
        first, second, old, draws = local[4 * n:4 * n + 4]
        if n == 0:
            scaled_copies[0].wait()
        copies(n, 0)().wait()
        update = mm(left_a[...], first[...], NT)
        if n == 0:
            scaled_copies[1].wait()
        copies(n, 1)().wait()
        update = update + mm(left_b[...], second[...], NT)
        copies(n, 2)().wait()
        schur = old[...] - update
        copies(n, 3)().wait()
        for t in range(pieces[n]):
            for i in range(tile_rows):
                tile = schur[i * size:(i + 1) * size, t * size:(t + 1) * size]
                tiles[at] = tile
                y = dot3(halves(draws[i, t]), halves(tile), NT)
                ranges[at] = y
                grams[at] = lax.dot_general(
                    y, y, NT, precision=lax.Precision.HIGHEST, preferred_element_type=jnp.float32
                )
                at += 1
    row_id = lax.broadcasted_iota(jnp.int32, (batch, rank, rank), 1)
    col_id = lax.broadcasted_iota(jnp.int32, (batch, rank, rank), 2)
    eye = jnp.where(row_id == col_id, 1.0, 0.0).astype(jnp.float32)
    work = jnp.concatenate([grams[...], eye], axis=2)
    rows = lax.broadcasted_iota(jnp.int32, (batch, rank, 1), 1)
    for k in range(rank):
        scale = lax.rsqrt(work[:, k:k + 1, k:k + 1])
        pivot_row = work[:, k:k + 1, :] * scale
        column = work[:, :, k:k + 1] * scale
        below = jnp.where(rows > k, column, 0.0)
        work = jnp.where(rows == k, pivot_row, work - below * pivot_row)
    inverse = work[:, :, rank:]
    at = 0
    for n in range(count):
        for t in range(pieces[n]):
            slot = meta[4 * n + 2] + t
            for i in range(tile_rows):
                u = lax.dot_general(
                    inverse[at], ranges[at], NN,
                    precision=lax.Precision.HIGHEST, preferred_element_type=jnp.float32,
                )
                out[0, i, slot] = u.astype(jnp.bfloat16)
                out[1, i, slot] = dot3(halves(u), halves(tiles[at]), NN).astype(jnp.bfloat16)
                at += 1


def compress(scaled, trailing, omega, parts):
    tile_rows, _, rank, size = omega.shape
    rows, width = trailing.shape
    pieces = tuple(part[3].shape[0] // size for part in parts)
    choices = tuple(len(part[0]) for part in parts)
    total = sum(pieces)
    meta = jnp.stack(
        [jnp.int32(0) + x for part in parts for x in (part[2], part[4], part[5], part[1])]
    ).astype(jnp.int32)
    out = jax.ShapeDtypeStruct((2, tile_rows, total, rank, size), jnp.bfloat16)
    batch = total * tile_rows
    operands = [*scaled, trailing, omega]
    count = len(operands)
    local = []
    for part, piece in zip(parts, pieces):
        operands += part[0]
        local += [
            pltpu.VMEM((piece * size, part[0][0].shape[1]), jnp.bfloat16),
            pltpu.VMEM(part[3].shape, jnp.bfloat16),
            pltpu.VMEM((rows, piece * size), jnp.float32),
            pltpu.VMEM((tile_rows, piece, rank, size), jnp.float32),
        ]
    operands += [part[3] for part in parts]
    return pl.pallas_call(
        functools.partial(compress_kernel, pieces=pieces, choices=choices),
        in_specs=[SMEM] + [HBM] * len(operands),
        out_specs=VMEM,
        out_shape=out,
        scratch_shapes=[pltpu.VMEM(x.shape, jnp.bfloat16) for x in scaled] + local + [
            pltpu.VMEM((batch, size, size), jnp.float32),
            pltpu.VMEM((batch, rank, size), jnp.float32),
            pltpu.VMEM((batch, rank, rank), jnp.float32),
            pltpu.SemaphoreType.DMA((2 + 4 * len(parts),)),
        ],
        compiler_params=pltpu.CompilerParams(vmem_limit_bytes=40 << 20),
        cost_estimate=pl.CostEstimate(
            flops=8 * rows * width * total * size, transcendentals=0, bytes_accessed=8 * rows * width
        ),
        name="compress",
    )(meta, *in_hbm(operands[:count]), *operands[count:])


def place_kernel(meta, maps, base, *refs, fronts, blocks, row_dev):
    count = len(blocks)
    packs = [refs[n * fronts:(n + 1) * fronts] for n in range(count)]
    out, *mine = refs[-(5 + count):-4]
    lines, left, right, sems = refs[-4:]
    _, tile_rows, _, rank, size = packs[0][0].shape
    steps, height, width = lines.shape
    per_block = row_dev // size
    group = per_block * rank
    depth = tile_rows * group
    spare = height - row_dev

    def fetch(n, slot, go):
        for offset in range(fronts):
            @pl.when(jnp.logical_and(meta[slot] >= 0, meta[KIDS + slot] == offset))
            def _():
                go(pltpu.make_async_copy(packs[n][offset], mine[n].at[slot], sems.at[n * KIDS + slot]))

    def columns(step):
        return pl.ds(pl.multiple_of(meta[2 * KIDS + 1 + step] * width, width), width)

    def load(step):
        return pltpu.make_async_copy(base.at[:, columns(step)], lines.at[step], sems.at[count * KIDS + step])

    def store(step):
        return pltpu.make_async_copy(lines.at[step], out.at[:, columns(step)], sems.at[count * KIDS + steps + step])

    def selection(panel, child, t):
        lane = pl.multiple_of(panel * row_dev + t * size, size)
        ids = maps[pl.ds(jnp.maximum(child, 0), 1), pl.ds(lane, size)] - t * size
        hit = lax.broadcasted_iota(jnp.int32, (size + spare, size), 0) == ids
        return jnp.where(hit, 1.0, 0.0).astype(jnp.bfloat16)

    for n in range(count):
        for slot in range(KIDS):
            fetch(n, slot, lambda copy: copy.start())
    for step in range(steps):
        load(step).start()
    left[...] = jnp.zeros(left.shape, left.dtype)
    right[...] = jnp.zeros(right.shape, right.dtype)
    for slot in range(KIDS):
        @pl.when(meta[slot] < 0)
        def _():
            for n in range(count):
                mine[n][slot] = jnp.zeros(mine[n].shape[1:], jnp.bfloat16)
    for n in range(count):
        for slot in range(KIDS):
            fetch(n, slot, lambda copy: copy.wait())
    for slot in range(KIDS):
        lo = slot * depth
        for i in range(tile_rows):
            source = jnp.concatenate(
                [mine[n][slot, 0, i].reshape(blocks[n] * group, size) for n in range(count)], axis=0
            )
            spread = mm(selection(meta[2 * KIDS], meta[slot], i), source, NT).astype(jnp.bfloat16)
            for step in range(steps):
                left[step, i * size:(i + 1) * size + spare, lo + i * group:lo + (i + 1) * group] = (
                    spread[:, step * group:(step + 1) * group]
                )

    step = 0
    for n in range(count):
        for b in range(blocks[n]):
            for slot in range(KIDS):
                lo = slot * depth
                for t in range(per_block):
                    source = jnp.concatenate(
                        [mine[n][slot, 1, i, b * per_block + t] for i in range(tile_rows)], axis=0
                    )
                    pick = selection(meta[2 * KIDS + 1 + step], meta[slot], t)
                    spread = mm(pick, source, NT).astype(jnp.bfloat16)
                    for i in range(tile_rows):
                        at = lo + i * group + t * rank
                        right[t * size:(t + 1) * size + spare, at:at + rank] = (
                            spread[:, i * rank:(i + 1) * rank]
                        )

            load(step).wait()
            lines[step] = (
                lines[step].astype(jnp.float32) + mm(left[step], right[...], NT)
            ).astype(jnp.bfloat16)
            store(step).start()
            step += 1
    for step in range(steps):
        store(step).wait()


def place(meta, extend_map, packs, base, row_dev, blocks, previous):
    fronts = len(packs[0])
    _, tile_rows, _, rank, size = packs[0][0].shape
    height, full = base.shape
    panels = extend_map.shape[1] // row_dev
    width = full // panels
    depth = KIDS * tile_rows * (row_dev // size) * rank
    steps = sum(blocks)
    operands = [base] + [x for chunk in packs for x in chunk]
    aliases = {}
    if previous is not None:
        operands.append(previous)
        aliases = {1 + len(operands): 0}
    return pl.pallas_call(
        functools.partial(place_kernel, fronts=fronts, blocks=blocks, row_dev=row_dev),
        in_specs=[SMEM, VMEM] + [HBM] * len(operands),
        out_specs=HBM,
        out_shape=jax.ShapeDtypeStruct(base.shape, base.dtype),
        scratch_shapes=[pltpu.VMEM((KIDS,) + chunk[0].shape, jnp.bfloat16) for chunk in packs] + [
            pltpu.VMEM((steps, height, width), jnp.bfloat16),
            pltpu.VMEM((steps, height, depth), jnp.bfloat16),
            pltpu.VMEM((width, depth), jnp.bfloat16),
            pltpu.SemaphoreType.DMA((len(packs) * KIDS + 2 * steps,)),
        ],
        input_output_aliases=aliases,
        compiler_params=pltpu.CompilerParams(vmem_limit_bytes=48 << 20),
        cost_estimate=pl.CostEstimate(
            flops=8 * height * width * steps * depth, transcendentals=0, bytes_accessed=4 * height * width * steps
        ),
        name="place",
    )(meta, extend_map, *in_hbm(operands[:1]), *operands[1:])


def spread_panels(x, lowest):
    held = {0: x}
    for bit in bits_of(lax.axis_size("panel"), lowest):
        for offset in list(held):
            held[offset ^ bit] = swap(held[offset], "panel", bit)
    return held


def gather_fronts(pack):
    held = {0: pack}
    for bit in bits_of(lax.axis_size("front"), 1):
        for offset in list(held):
            held[offset ^ bit] = swap(held[offset], "front", bit)
    return [held[offset] for offset in range(len(held))]


def body(coupling, pivot_inverse, pivots, trailing, sketch, extend_map, parent_of, parent_base):
    rows_here = coupling[0]
    inverse = pivot_inverse[0]
    row_dev, width = rows_here.shape
    omega = sketch[0]
    size = omega.shape[3]
    panels = lax.axis_size("panel")
    panel_here = lax.axis_index("panel").astype(jnp.int32)
    owner = lax.axis_index("front").astype(jnp.int32)
    core = panel_here & 1
    per_block = row_dev // size
    middle = inverse.shape[1] // 2

    near_inverse = swap(inverse, "panel", 1)
    held_a = spread_panels(inverse[:, :middle], 2)
    held_b = spread_panels(lax.optimization_barrier(inverse)[:, middle:], 2)
    offsets = range(panels)
    panel_of = jnp.stack([panel_here ^ offset for offset in offsets])

    def arrivals(held):
        parts = []
        for offset in offsets[2:]:
            if offset & 1:
                parts.append(swap(held[offset ^ 1], "panel", 1))
            else:
                parts.append(held[offset])
        return parts

    factor_a, scaled_a = factor_columns(
        panel_of, rows_here, [inverse, near_inverse] + arrivals(held_a), 0, middle, pivots=pivots
    )
    far_a = spread_panels(factor_a, 2)
    near_a = {offset ^ 1: swap(x, "panel", 1) for offset, x in far_a.items()}
    first = {**far_a, **near_a}
    early = factor_columns(panel_of[:2], rows_here, [inverse, near_inverse], middle, width - middle)
    factor_b, scaled_b = factor_columns(
        panel_of[2:], rows_here, arrivals(held_b), middle, width - middle, early, pivots
    )
    near_b = swap(factor_b, "panel", 1)
    scaled = (scaled_a, scaled_b)

    fronts = parent_of.shape[0]
    mine = parent_of == owner
    rank_of = jnp.cumsum(mine.astype(jnp.int32)) - 1
    slots = jnp.arange(KIDS, dtype=jnp.int32)
    match = mine[None, :] & (rank_of[None, :] == slots[:, None])
    child = jnp.sum(jnp.where(match, jnp.arange(fronts, dtype=jnp.int32)[None, :] + 1, 0), axis=1) - 1
    slot_meta = jnp.concatenate([child, jnp.maximum(child, 0) ^ owner, panel_here[None]]).astype(jnp.int32)

    mate = panel_here ^ 1
    chunks = [(
        [panel_here, mate],
        [
            ([factor_a], 0, 0, factor_b, panel_here * per_block, 0),
            ([first[1]], 0, 0, near_b, mate * per_block, per_block),
        ],
    )]
    if per_block % 2 == 0:
        half = row_dev // 2
        tiles = per_block // 2
        pieces = []
        for c in range(2):
            chosen = jnp.where(
                core == c,
                lax.dynamic_slice_in_dim(factor_b, core * half, half, 0),
                lax.dynamic_slice_in_dim(near_b, core * half, half, 0),
            )
            pieces.append(spread_panels(chosen, 2))
        for offset in sorted(pieces[0])[1:]:
            for c in range(2):
                here = pieces[c][offset]
                there = swap(here, "panel", 1)
                block = ((panel_here ^ offset) & ~1) + c
                both = [first[offset], first[offset ^ 1]]
                parts = [
                    (both, core ^ c, x * tiles, piece, block * per_block + x * tiles, x * tiles)
                    for x, piece in ((core, here), (1 - core, there))
                ]
                chunks.append(([block], parts))
    else:
        held = spread_panels(factor_b, 2)
        for offset in sorted(held)[1:]:
            block = panel_here ^ offset
            there = swap(held[offset], "panel", 1)
            chunks.append((
                [block, block ^ 1],
                [
                    ([first[offset]], 0, 0, held[offset], block * per_block, 0),
                    ([first[offset ^ 1]], 0, 0, there, (block ^ 1) * per_block, per_block),
                ],
            ))

    packs = []
    for _, parts in chunks:
        packs.append(compress(scaled, trailing[0], omega, parts))
    gathered = []
    for pack in packs:
        gathered.append(gather_fronts(pack))
    assembled = None
    for picked in (slice(0, 1), slice(1, None)):
        steps = [block for blocks, _ in chunks[picked] for block in blocks]
        meta = jnp.concatenate([slot_meta, jnp.stack(steps).astype(jnp.int32)])
        counts = tuple(len(blocks) for blocks, _ in chunks[picked])
        assembled = place(meta, extend_map, gathered[picked], parent_base[0], row_dev, counts, assembled)
    return assembled[None]


def solution(mesh):
    placed = (
        P("front", "panel", None),
        P("front", "panel", None),
        P("front", None),
        P("front", "panel", None),
        P("front", "panel", None, None, None),
        P(),
        P(),
        P("front", "panel", None),
    )
    return jax.shard_map(body, mesh=mesh, in_specs=placed, out_specs=P("front", "panel", None), check_vma=False)
```
